32 devices in a mesh: row: 8 (over z, y), col: 4 (over x, core).
Axes of the slice: x: 2, y: 2, z: 4, core: 2. Of those that a mesh axis runs over, the one named last changes fastest.
Arguments:
- tile_seeds: int32 [32, 8, 64, 4], P(None, 'row', None, 'col'), may hold values from 0 to 1073741823
- factors: bfloat16 [32, 1024, 64, 512], P(None, 'row', None, 'col'), may hold values from -0.015625 to 0.015625
- lower_inverse: bfloat16 [4, 16, 512, 8, 1024], P(None, None, 'col', None, 'row'), may hold values from -0.1 to 2
- upper_inverse: bfloat16 [4, 16, 512, 8, 1024], P(None, None, 'col', None, 'row'), may hold values from -0.1 to 2
- right_side: float32 [32, 1024], P(None, 'row'), may hold values from -6 to 6
- first_guess: float32 [64, 512], P(None, 'col'), may hold values from -6 to 6
Outputs:
- solution: float32 [64, 512], P(None, 'col')
- hessenberg: float32 [4, 3], replicated
The draws below stay inside these ranges and needn't reach their ends.
All inputs are finite; a program needn't handle non-finite values.
Results may differ from the reference program's by a relative error of at most 0.011.
Values may be sent and summed in bfloat16 or wider, within the bound.
No kernel may reach another device: no remote copies, remote signals or barrier semaphores. Data moves between devices by JAX's collectives and lax.ppermute only.
A program may use at most 320 MiB of HBM per device.

```python
import jax
import jax.numpy as jnp
from jax import lax

ORDER = 32768
TILE = 128
SWEEPS = 4
ITERS = 3
DIAG_ORDER = 8192
N_ROW = 8
N_COL = 4


def inverse_blocks(key):
    diag_key, coupling_key = jax.random.split(key)
    shape = (SWEEPS, DIAG_ORDER, DIAG_ORDER)
    diagonal = jax.random.uniform(diag_key, (SWEEPS, DIAG_ORDER), jnp.float32, 0.6, 1.4)
    coupling = jax.random.truncated_normal(coupling_key, -4.0, 4.0, shape, jnp.float32) * (0.3 * DIAG_ORDER ** (-0.5))
    identity_mask = jnp.eye(DIAG_ORDER, dtype=bool)
    blocks = jnp.where(identity_mask[None], diagonal[:, :, None], coupling)
    return blocks.reshape(SWEEPS, DIAG_ORDER // (TILE * N_COL), TILE * N_COL, DIAG_ORDER // (TILE * N_ROW), TILE * N_ROW).astype(jnp.bfloat16)


def draw_lower_inverse(key, part):
    return inverse_blocks(jax.random.fold_in(key, 11))


def draw_upper_inverse(key, part):
    return inverse_blocks(jax.random.fold_in(key, 23))


def set_ends(values, rng, least, largest):
    place = [jax.random.randint(jax.random.fold_in(rng, axis), (), 0, length) for axis, length in enumerate(values.shape)]
    widest = values.shape.index(max(values.shape))
    beside = place[:widest] + [(place[widest] + 1) % values.shape[widest]] + place[widest + 1:]
    return values.at[tuple(place)].set(least).at[tuple(beside)].set(largest)


def block_levels(key, shape, shards, least, top_value):
    def one(axis_at, shards_of):
        draws = jax.random.uniform(jax.random.fold_in(jax.random.fold_in(key, 6), axis_at), (shards_of,), jnp.float32, least / len(shards), top_value / len(shards))
        return jnp.repeat(jnp.exp(draws), shape[axis_at] // shards_of).reshape((-1,) + (1,) * (len(shape) - axis_at - 1))

    loudness = one(*shards[0])
    for cut in shards[1:]:
        loudness = loudness * one(*cut)
    return loudness


def normal_values(rng, shape, width, most, shards=(), kind=jnp.bfloat16):
    result = jax.random.normal(rng, shape, jnp.float32) * width
    if len(shards) > 0:
        result = block_levels(rng, shape, shards, -0.22, 0.18) * result
    return jnp.clip(result, min=-most, max=most).astype(kind)


def setup_inputs(seed: int = 0) -> dict:
    arg_keys = jax.random.split(jax.random.key(seed), 7)
    return {
        "tile_seeds": set_ends(jax.random.randint(arg_keys[0], (ORDER // (TILE * N_ROW), N_ROW, ORDER // (TILE * N_COL), N_COL), 0, 1073741824), jax.random.fold_in(arg_keys[0], 1), 0, 1073741823).astype(jnp.int32),
        "factors": normal_values(arg_keys[1], (ORDER // (TILE * N_ROW), TILE * N_ROW, ORDER // (TILE * N_COL), TILE * N_COL), (4 * ORDER) ** -0.5, 0.015625, ((1, 8), (3, 4))),
        "lower_inverse": draw_lower_inverse(jax.random.fold_in(arg_keys[6], 71), 0),
        "upper_inverse": draw_upper_inverse(jax.random.fold_in(arg_keys[6], 71), 0),
        "right_side": normal_values(arg_keys[4], (ORDER // (TILE * N_ROW), TILE * N_ROW), 1.0, 6.0, ((1, 8),), jnp.float32),
        "first_guess": normal_values(arg_keys[5], (ORDER // (TILE * N_COL), TILE * N_COL), 0.5, 6.0, ((1, 4),), jnp.float32),
    }


DIAG_SHIFT = 2.0

def scrambled(tile_seed, flat_index):
    hashed = tile_seed + flat_index * 1640531527
    hashed = hashed ^ hashed >> 16 & 65535
    hashed = hashed * 2146121005
    hashed = hashed ^ hashed >> 15 & 131071
    hashed = hashed * 1779033703
    hashed = hashed ^ hashed >> 16 & 65535
    high_bits = hashed >> 8 & 16777215
    return (high_bits.astype(jnp.float32) - 8388607.5) / 8388608.0

def small_solve(normal_matrix, target):
    factor = jnp.linalg.cholesky(normal_matrix)
    order_small = normal_matrix.shape[0]
    forward = []
    for position in range(order_small):
        partial_value = target[position]
        for earlier in range(position):
            partial_value = partial_value - factor[position, earlier] * forward[earlier]
        forward.append(partial_value / factor[position, position])
    backward = [None] * order_small
    for position in reversed(range(order_small)):
        partial_value = forward[position]
        for after_pos in range(position + 1, order_small):
            partial_value = partial_value - factor[after_pos, position] * backward[after_pos]
        backward[position] = partial_value / factor[position, position]
    return backward

def matrix_times(seed_grid, vector):
    tile_count = ORDER // TILE
    offsets = jnp.arange(TILE, dtype=jnp.int32)
    flat_index = offsets[:, None] * TILE + offsets[None, :]
    shaped = vector.reshape(tile_count, TILE)
    entry_scale = ORDER ** (-0.5)

    def one_row(seed_row):
        values = scrambled(seed_row[None, :, None], flat_index[:, None, :]) * entry_scale
        return jnp.einsum('icj,cj->i', values, shaped, precision=lax.Precision.HIGHEST)
    return lax.map(one_row, seed_grid).reshape(ORDER) + DIAG_SHIFT * vector

def lower_sweep(matrix, lower_blocks, vector):
    solved = []
    for sweep_step in range(SWEEPS):
        first_row = sweep_step * DIAG_ORDER
        target = vector[first_row:first_row + DIAG_ORDER]
        if sweep_step > 0:
            earlier = jnp.concatenate(solved).astype(jnp.bfloat16)
            target = target - jnp.dot(matrix[first_row:first_row + DIAG_ORDER, :first_row].astype(jnp.float32), earlier.astype(jnp.float32), preferred_element_type=jnp.float32)
        solved.append(jnp.dot(lower_blocks[sweep_step].astype(jnp.float32), target.astype(jnp.bfloat16).astype(jnp.float32), preferred_element_type=jnp.float32))
    return jnp.concatenate(solved)

def upper_sweep(matrix, upper_blocks, vector):
    solved = [None] * SWEEPS
    for sweep_step in reversed(range(SWEEPS)):
        first_row = sweep_step * DIAG_ORDER
        next_row = first_row + DIAG_ORDER
        target = vector[first_row:next_row]
        if sweep_step < SWEEPS - 1:
            later_part = jnp.concatenate(solved[sweep_step + 1:]).astype(jnp.bfloat16)
            target = target - jnp.dot(matrix[first_row:next_row, next_row:].astype(jnp.float32), later_part.astype(jnp.float32), preferred_element_type=jnp.float32)
        solved[sweep_step] = jnp.dot(upper_blocks[sweep_step].astype(jnp.float32), target.astype(jnp.bfloat16).astype(jnp.float32), preferred_element_type=jnp.float32)
    return jnp.concatenate(solved)

def reference(tile_seeds, factors, lower_inverse, upper_inverse, right_side, first_guess):
    tile_count = ORDER // TILE
    seed_grid = tile_seeds.reshape(tile_count, tile_count)
    matrix = factors.reshape(ORDER, ORDER)
    lower_blocks = lower_inverse.reshape(SWEEPS, DIAG_ORDER, DIAG_ORDER)
    upper_blocks = upper_inverse.reshape(SWEEPS, DIAG_ORDER, DIAG_ORDER)
    start_point = first_guess.reshape(ORDER)
    residual = right_side.reshape(ORDER) - matrix_times(seed_grid, start_point)
    initial_norm = jnp.sqrt(jnp.sum(residual * residual))
    basis_list = [residual / initial_norm]
    directions = []
    hessenberg = jnp.zeros((ITERS + 1, ITERS), jnp.float32)
    for column in range(ITERS):
        lowered = lower_sweep(matrix, lower_blocks, basis_list[column])
        direction = upper_sweep(matrix, upper_blocks, lowered)
        directions.append(direction)
        mapped = matrix_times(seed_grid, direction)
        coeffs = jnp.stack([jnp.sum(vector * mapped) for vector in basis_list])
        for position in range(column + 1):
            mapped = mapped - coeffs[position] * basis_list[position]
        length = jnp.sqrt(jnp.sum(mapped * mapped))
        hessenberg = hessenberg.at[:column + 1, column].set(coeffs).at[column + 1, column].set(length)
        if column + 1 < ITERS:
            basis_list.append(mapped / length)
    normal_matrix = jnp.dot(hessenberg.T, hessenberg, precision=lax.Precision.HIGHEST)
    weights = small_solve(normal_matrix, initial_norm * hessenberg[0])
    solution = start_point
    for position in range(ITERS):
        solution = solution + weights[position] * directions[position]
    return (solution.reshape(ORDER // (TILE * N_COL), TILE * N_COL), hessenberg)
```

```python
import functools

import jax
import jax.numpy as jnp
from jax import lax
from jax.experimental import pallas as pl
from jax.experimental.pallas import tpu as pltpu
from jax.sharding import PartitionSpec as P

ITERS = 3
DIAG_SHIFT = 2.0
F32 = jnp.float32
BF16 = jnp.bfloat16
LANES = 128
NT = (((1,), (1,)), ((), ()))
VMEM_LIMIT = 24 << 20
COST_RATE = 5e8


def split_rows(row):
    wide = jnp.broadcast_to(row, (16, row.shape[1]))
    high = wide.astype(BF16).astype(F32)
    at = lax.broadcasted_iota(jnp.int32, wide.shape, 0)
    return jnp.where(at == 0, high, jnp.where(at == 1, wide - high, 0.0)).astype(BF16)


def hashed(seed, step):
    h = seed + step
    h = h ^ lax.shift_right_logical(h, 16)
    h = h * 2146121005
    h = h ^ lax.shift_right_logical(h, 15)
    h = h * 1779033703
    h = h ^ lax.shift_right_logical(h, 16)
    return h ^ jnp.int32(-2147483648)


def generate_body(n_rows, seeds, table, x_ref, a_ref, y_ref):
    step = pl.program_id(0)

    @pl.when(step == 0)
    def _():
        y_ref[...] = jnp.zeros_like(y_ref)

    def tiles(at, carry):
        for half in range(2):
            m = 2 * at + half
            for q in range(2):
                seed = seeds[m, 2 * step + q]
                for part in range(4):
                    rows = pl.ds(part * 32, 32)
                    h = hashed(seed, table[rows, :])
                    a_ref[pl.ds(q * LANES + part * 32, 32), pl.ds(m * LANES, LANES)] = h.astype(F32).astype(BF16)
        return carry

    lax.fori_loop(0, n_rows // 2, tiles, 0)
    left = jnp.concatenate([split_rows(x_ref[pl.ds(2 * step + q, 1), :]) for q in range(2)], axis=1)
    y_ref[...] += jnp.dot(left, a_ref[...], preferred_element_type=F32)


def generate(seeds, table, x_col):
    n_rows, n_cols = seeds.shape
    wide = n_rows * LANES
    return pl.pallas_call(
        functools.partial(generate_body, n_rows),
        grid=(n_cols // 2,),
        in_specs=[
            pl.BlockSpec(memory_space=pltpu.SMEM),
            pl.BlockSpec((LANES, LANES), lambda g: (0, 0)),
            pl.BlockSpec((n_cols, LANES), lambda g: (0, 0)),
        ],
        out_specs=[
            pl.BlockSpec((2 * LANES, wide), lambda g: (g, 0)),
            pl.BlockSpec((16, wide), lambda g: (0, 0)),
        ],
        out_shape=[
            jax.ShapeDtypeStruct((n_cols * LANES, wide), BF16),
            jax.ShapeDtypeStruct((16, wide), F32),
        ],
        compiler_params=pltpu.CompilerParams(vmem_limit_bytes=32 << 20),
        name="generate",
    )(seeds, table, x_col)


def cost(micros):
    return pl.CostEstimate(flops=int(micros * COST_RATE), bytes_accessed=int(micros * 3e6), transcendentals=0)


def vmem_spec():
    return pl.BlockSpec(memory_space=pltpu.VMEM)


def fetched(refs, buffers, sem):
    copies = [pltpu.make_async_copy(ref, buffer, sem.at[at]) for at, (ref, buffer) in enumerate(zip(refs, buffers))]
    for copy in copies:
        copy.start()
    return copies


def small_scratch(smalls):
    return [pltpu.VMEM(x.shape, x.dtype) for x in smalls] + [pltpu.SemaphoreType.DMA((len(smalls),))]


def any_spec():
    return pl.BlockSpec(memory_space=pl.ANY)


def apply_body(steps, first, slots, scale, last, n_small, place, *refs):
    smalls, a_ref, y_ref = refs[:n_small], refs[n_small], refs[n_small + 1]
    buffers, small_sem = refs[n_small + 2 : 2 * n_small + 2], refs[2 * n_small + 2]
    acc, z_all, held, sems = refs[2 * n_small + 3 :]
    chunk = held.shape[1]
    tiles = chunk // LANES

    def copy(at):
        slot = lax.rem(at, slots)
        return pltpu.make_async_copy(a_ref.at[pl.ds((first * steps + at) * chunk, chunk), :], held.at[slot], sems.at[slot])

    waits = fetched(smalls, buffers, small_sem)
    for at in range(min(slots - 1, steps)):
        copy(at).start()
    for wait in waits:
        wait.wait()
    z_ref, rest = buffers[0], buffers[1:]
    if first < last:
        acc[...] = rest[0][...]
        rest = rest[1:]
    else:
        acc[...] = jnp.zeros_like(acc)
    z_all[...] = jnp.sum(z_ref[...], axis=0)

    def body(at, carry):
        @pl.when(at + slots - 1 < steps)
        def _():
            copy(at + slots - 1).start()

        left = jnp.concatenate([split_rows(z_all[pl.ds(tiles * at + q, 1), :]) for q in range(tiles)], axis=1)
        copy(at).wait()
        acc[...] += jnp.dot(left, held[lax.rem(at, slots)], preferred_element_type=F32)
        return carry

    lax.fori_loop(0, steps, body, 0)
    if first > 0:
        y_ref[...] = acc[...]
        return
    total = acc[0:1, :] + acc[1:2, :]
    for m in range(y_ref.shape[0]):
        y_ref[m : m + 1, :] = total[:, m * LANES : (m + 1) * LANES] * scale
    count = y_ref.shape[0] // (last + 1)
    spread = z_all.shape[0] // count
    for at, ref in enumerate(rest):
        y_ref[(at + 1) * count : (at + 2) * count, :] += DIAG_SHIFT * ref[...]
    mine = z_all[pl.ds(place[0], count, stride=spread), :]
    y_ref[0:count, :] += jnp.where(place[1] == 1, DIAG_SHIFT, 0.0) * mine


def apply_block(a, parts, block, blocks, prior, owns, place, scale):
    depth, wide = a.shape
    span = depth // blocks
    chunk = min(256, span)
    slots = min(8, span // chunk)
    smalls = [parts] + prior + owns
    return pl.pallas_call(
        functools.partial(apply_body, span // chunk, block, slots, scale, blocks - 1, len(smalls)),
        in_specs=[pl.BlockSpec(memory_space=pltpu.SMEM)] + [any_spec()] * (len(smalls) + 1),
        out_specs=vmem_spec(),
        out_shape=jax.ShapeDtypeStruct((wide // LANES, LANES) if block == 0 else (16, wide), F32),
        scratch_shapes=small_scratch(smalls)
        + [
            pltpu.VMEM((16, wide), F32),
            pltpu.VMEM(parts.shape[1:], F32),
            pltpu.VMEM((slots, chunk, wide), BF16),
            pltpu.SemaphoreType.DMA((slots,)),
        ],
        compiler_params=pltpu.CompilerParams(vmem_limit_bytes=VMEM_LIMIT),
        cost_estimate=cost(6.0),
        name="apply_block",
    )(place, *smalls, a)


def rows_body(count, n, source, n_small, prepare, finish, *refs):
    operands, w_ref, out_ref = refs[:n_small], refs[n_small], refs[n_small + 1]
    smalls, small_sem = refs[n_small + 2 : 2 * n_small + 2], refs[2 * n_small + 2]
    scratch_a, scratch_b, totals = refs[2 * n_small + 3 : 2 * n_small + 6]
    group = min(n, 8)
    chunk = 16
    waits = fetched(operands, smalls, small_sem)
    near = len(refs) == 2 * n_small + 6
    if near:
        held = w_ref
    else:
        held, sems = refs[2 * n_small + 6 :]

        def copy(at):
            return pltpu.make_async_copy(source(w_ref, at), held.at[at], sems.at[at])

        for at in range(count):
            copy(at).start()
    for wait in waits:
        wait.wait()
    vec = prepare(*smalls)

    def multiply(at, scratch):
        if not near:
            copy(at).wait()
        for part in range(LANES // chunk):
            if len(held.shape) == 3:
                w = held[at, pl.ds(part * chunk * n, chunk * n), :].astype(F32).reshape(chunk, n, LANES)
            else:
                w = held[at, pl.ds(part * chunk, chunk), :, :].astype(F32)
            p = w * vec[None]
            if n > 8:
                p = jnp.sum(p.reshape(chunk, n // 8, 8, LANES), axis=1)
            scratch[pl.ds(part * chunk * group, chunk * group), :] = p.reshape(chunk * group, LANES)

    def add_up(at, scratch):
        total = scratch[pl.ds(0, LANES, stride=group), :]
        for q in range(1, group):
            total = total + scratch[pl.ds(q, LANES, stride=group), :]
        high = total.astype(BF16)
        at = pl.ds(at * LANES, LANES)
        totals[at, 0:LANES] = high
        totals[at, LANES : 2 * LANES] = (total - high.astype(F32)).astype(BF16)

    def body(at, carry):
        multiply(2 * at, scratch_a)

        @pl.when(at > 0)
        def _():
            add_up(2 * at - 1, scratch_b)

        multiply(2 * at + 1, scratch_b)
        add_up(2 * at, scratch_a)
        return carry

    lax.fori_loop(0, count // 2, body, 0)
    add_up(count - 1, scratch_b)
    ones = jnp.ones((16, 2 * LANES), BF16)
    out = lax.dot_general(ones, totals[...], NT, preferred_element_type=F32)
    finish(out_ref, [out[0:1, at * LANES : (at + 1) * LANES] for at in range(count)], *smalls)


def rows_product(w, smalls, n, count, source, prepare, finish, out_shape, name, micros):
    near = not callable(source)
    group = min(n, 8)
    return pl.pallas_call(
        functools.partial(rows_body, count, n, source, len(smalls), prepare, finish),
        in_specs=[any_spec()] * len(smalls) + [vmem_spec() if near else any_spec()],
        out_specs=vmem_spec(),
        out_shape=jax.ShapeDtypeStruct(out_shape, F32),
        scratch_shapes=small_scratch(smalls)
        + [
            pltpu.VMEM((LANES * group, LANES), F32),
            pltpu.VMEM((LANES * group, LANES), F32),
            pltpu.VMEM((count * LANES, 2 * LANES), BF16),
        ]
        + ([] if near else [pltpu.VMEM((count, LANES, n, LANES), BF16), pltpu.SemaphoreType.DMA((count,))]),
        compiler_params=pltpu.CompilerParams(vmem_limit_bytes=VMEM_LIMIT),
        cost_estimate=cost(micros),
        name=name,
    )(*smalls, w)


def rounded(x):
    return x.astype(BF16).astype(F32)


def orthonormalize_body(tiles, n_basis, got_ref, w_ref, *rest):
    basis, firsts, (v_ref, first_ref, sums_ref) = rest[:n_basis], rest[n_basis : 2 * n_basis], rest[-3:]
    got = jnp.sum(got_ref[...], axis=0)
    sums = jnp.broadcast_to(jnp.sum(got[tiles : tiles + 8], axis=1, keepdims=True), (8, LANES))
    w = w_ref[...]
    first = got[:tiles]
    square = sums[n_basis : n_basis + 1, :]
    for at in range(n_basis):
        h = sums[at : at + 1, :]
        square = square - h * h
        w = w - h * basis[at][...]
        first = first - h * firsts[at][...]
    length = jnp.sqrt(square)
    v_ref[...] = w / length
    first_ref[...] = first / length
    row = lax.broadcasted_iota(jnp.int32, (8, LANES), 0)
    sums_ref[...] = jnp.where(row == n_basis, length, sums)


def orthonormalize(got, w, basis, firsts, tiles):
    return pl.pallas_call(
        functools.partial(orthonormalize_body, tiles, len(basis)),
        in_specs=[vmem_spec()] * (2 + 2 * len(basis)),
        out_specs=[vmem_spec()] * 3,
        out_shape=[
            jax.ShapeDtypeStruct(w.shape, F32),
            jax.ShapeDtypeStruct((tiles, LANES), F32),
            jax.ShapeDtypeStruct((8, LANES), F32),
        ],
        name="orthonormalize",
    )(got, w, *basis, *firsts)


def small_solve(normal_matrix, target):
    size = normal_matrix.shape[0]
    factor = [[None] * size for _ in range(size)]
    for i in range(size):
        for j in range(i + 1):
            value = normal_matrix[i, j]
            for k in range(j):
                value = value - factor[i][k] * factor[j][k]
            factor[i][j] = jnp.sqrt(value) if i == j else value / factor[j][j]
    forward = []
    for i in range(size):
        value = target[i]
        for j in range(i):
            value = value - factor[i][j] * forward[j]
        forward.append(value / factor[i][i])
    backward = [None] * size
    for i in reversed(range(size)):
        value = forward[i]
        for j in range(i + 1, size):
            value = value - factor[j][i] * backward[j]
        backward[i] = value / factor[i][i]
    return backward


def shards(tile_seeds, factors, lower_inverse, upper_inverse, right_side, first_guess):
    n_row = lax.axis_size("row")
    n_col = lax.axis_size("col")
    row_index = lax.axis_index("row")
    col_index = lax.axis_index("col")
    seeds = tile_seeds[:, 0, :, 0]
    n_rows, n_cols = seeds.shape
    order = n_rows * n_row * LANES
    sweeps = lower_inverse.shape[0]
    rows_per = n_rows // sweeps
    cols_per = n_cols // sweeps
    spread = n_row // n_col
    scale = 2.0**-31 * order**-0.5
    has_own = (row_index % n_col == col_index).astype(F32)

    def own(col_part):
        tiles = col_part.reshape(-1, spread, LANES)
        return has_own * lax.dynamic_index_in_dim(tiles, row_index // n_col, 1, keepdims=False)

    def reduce_col(x):
        moved = [lax.ppermute(x, "col", [(i, (i + s) % n_col) for i in range(n_col)]) for s in range(1, n_col)]
        return functools.reduce(jnp.add, moved, x)

    def spread_col(x):
        moved = [lax.ppermute(x, "col", [(i, (i + s) % n_col) for i in range(n_col)]) for s in range(1, n_col)]
        return [x] + moved

    def spread_row(x):
        return lax.all_to_all(x, "row", 0, 0)

    j_index = jnp.arange(LANES, dtype=jnp.int32)
    table = (j_index[None, :] * LANES + j_index[:, None]) * 1640531527

    def finish(y, z):
        part = (y[0] + y[1]).reshape(n_rows, LANES)
        return part * scale + DIAG_SHIFT * own(z)

    def flat(inverse):
        return [inverse[k].reshape(cols_per, LANES * rows_per, LANES) for k in range(sweeps)]

    lower_flat, upper_flat = flat(lower_inverse), flat(upper_inverse)
    place = jnp.stack([row_index // n_col, (row_index % n_col == col_index).astype(jnp.int32)]).astype(jnp.int32)

    def copies(out_ref, rows, *smalls):
        for r in range(n_row):
            for at, row in enumerate(rows):
                out_ref[r, at : at + 1, :] = row

    def inverse_product(inverse, k, smalls, prepare, name):
        return rows_product(
            inverse[k],
            smalls,
            rows_per,
            cols_per,
            None,
            prepare,
            copies,
            (n_row, cols_per, LANES),
            name,
            3.0,
        )

    def factor_product(k, first, solved, extras, signs, micros):
        n_parts = len(solved)

        def prepare(*smalls):
            vecs = []
            for ref in smalls[:n_parts]:
                vecs.append(rounded(ref[...] if len(ref.shape) == 2 else jnp.sum(ref[...], axis=0)))
            return vecs[0] if n_parts == 1 else jnp.concatenate(vecs, axis=0)

        def finish(out_ref, rows, *smalls):
            for at, row in enumerate(rows):
                total = signs[-1] * row
                for sign, ref in zip(signs, smalls[n_parts:]):
                    total = total + sign * ref[at : at + 1, :]
                out_ref[at : at + 1, :] = total

        return rows_product(
            factors,
            list(solved) + list(extras),
            n_parts * cols_per,
            rows_per,
            lambda w, at: w.at[k * rows_per + at, :, pl.ds(first * cols_per, n_parts * cols_per), :],
            prepare,
            finish,
            (rows_per, LANES),
            "factors",
            micros,
        )

    def sums_rows(basis, w):
        rows = [jnp.sum(v * w, axis=0, keepdims=True) for v in basis + [w]]
        return jnp.concatenate(rows + [jnp.zeros((8 - len(rows), LANES), F32)], axis=0)

    def first_product(w, basis):
        n_basis = len(basis)

        def prepare(w_ref, *_):
            return w_ref[0:rows_per, :]

        def finish(out_ref, rows, w_ref, *basis_refs):
            tail = sums_rows([ref[...] for ref in basis_refs], w_ref[...])
            copies(out_ref, rows)
            for r in range(n_row):
                out_ref[r, cols_per:, :] = tail

        return rows_product(
            lower_flat[0],
            [w] + basis,
            rows_per,
            cols_per,
            None,
            prepare,
            finish,
            (n_row, cols_per + 8, LANES),
            "lower_inverse",
            3.0,
        )

    def added(parts):
        return functools.reduce(jnp.add, parts)

    matrix, y = generate(seeds, table, first_guess)
    w = right_side - reduce_col(finish(y, first_guess))
    basis, firsts, directions, columns = [], [], [], []
    for column in range(ITERS):
        got = spread_row(first_product(w, basis))
        vector, first, sums = orthonormalize(got, w, basis, firsts, cols_per)
        columns.append(sums)
        basis.append(vector)
        firsts.append(first)
        solved = [first]
        early = None
        for k in range(1, sweeps):
            if early is None:
                part = factor_product(k, k - 1, solved[k - 1 :], [], [1.0], 3.0)
            else:
                part = factor_product(k, k - 1, solved[k - 1 :], [early], [1.0, 1.0], 3.0)
            parts = spread_col(part)

            def prepare(v_ref, *part_refs, k=k):
                return rounded(v_ref[k * rows_per : (k + 1) * rows_per, :] - added([ref[...] for ref in part_refs]))

            product = inverse_product(lower_flat, k, [vector] + parts, prepare, "lower_inverse")
            product, solved = lax.optimization_barrier((product, solved))
            got = spread_row(product)
            if k + 1 < sweeps:
                early = factor_product(k + 1, 0, solved, [], [1.0], 2.0 * k + 1.0)
            solved.append(got)
        lowered = [own(first)] + [own(jnp.sum(got, axis=0)) for got in solved[1:]]
        solved = [None] * sweeps
        owns = [None] * sweeps
        early = None
        mapped = []
        for k in reversed(range(sweeps)):
            if k == sweeps - 1:
                part = lowered[k]
            elif early is None:
                part = factor_product(k, k + 1, solved[k + 1 : k + 2], [lowered[k]], [1.0, -1.0], 3.0)
            else:
                part = factor_product(k, k + 1, solved[k + 1 : k + 2], [lowered[k], early], [1.0, -1.0, -1.0], 3.0)
            if 0 < k < sweeps - 1:
                part, later = lax.optimization_barrier((part, solved[k + 1 :]))
                parts = spread_col(part)
                early = factor_product(k - 1, k + 1, later, [], [1.0], 2.0 * (sweeps - 1 - k) + 1.0)
                parts, early = lax.optimization_barrier((parts, early))
            else:
                parts = spread_col(part)

            def prepare(*part_refs):
                return rounded(added([ref[...] for ref in part_refs]))

            product = inverse_product(upper_flat, k, parts, prepare, "upper_inverse")
            if k < sweeps - 1:
                product, later = lax.optimization_barrier((product, solved[k + 1]))
                got = spread_row(product)
                mapped = [apply_block(matrix, later, k + 1, sweeps, mapped, [], place, scale)]
                owns[k + 1] = own(jnp.sum(later, axis=0))
                solved[k] = got
            else:
                solved[k] = spread_row(product)
        part = apply_block(matrix, solved[0], 0, sweeps, mapped, owns[1:], place, scale)
        directions.append(jnp.concatenate([jnp.sum(got, axis=0) for got in solved], axis=0))
        w = added(spread_col(part))
    got = spread_row(jnp.broadcast_to(sums_rows(basis, w)[None], (n_row, 8, LANES)))
    sums = jnp.sum(got, axis=(0, 2))
    lengths = [columns[k][k, 0] for k in range(ITERS)]
    initial_norm = lengths[0]
    heights = [[columns[k][j, 0] for j in range(k)] + [lengths[k]] for k in range(1, ITERS)]
    last = [sums[j] for j in range(ITERS)]
    heights.append(last + [jnp.sqrt(functools.reduce(lambda a, h: a - h * h, last, sums[ITERS]))])
    zero = jnp.zeros((), F32)
    hessenberg = jnp.stack([jnp.stack(c + [zero] * (ITERS + 1 - len(c))) for c in heights], axis=1)
    normal_matrix = jnp.dot(hessenberg.T, hessenberg, precision=lax.Precision.HIGHEST)
    weights = small_solve(normal_matrix, initial_norm * hessenberg[0])
    solution = first_guess
    for position in range(ITERS):
        solution = solution + weights[position] * directions[position]
    return (solution, hessenberg)


def solution(mesh):
    in_specs = (
        P(None, "row", None, "col"),
        P(None, "row", None, "col"),
        P(None, None, "col", None, "row"),
        P(None, None, "col", None, "row"),
        P(None, "row"),
        P(None, "col"),
    )
    out_specs = (P(None, "col"), P())
    return jax.shard_map(shards, mesh=mesh, in_specs=in_specs, out_specs=out_specs, check_vma=False)
```
